32 devices in a mesh: ens: 4 (over y, x), slab: 8 (over z, core).
Axes of the slice: x: 2, y: 2, z: 4, core: 2. Of those that a mesh axis runs over, the one named last changes fastest.
Arguments:
- density0: float32 [192, 1024], P('slab'), may hold values from 0.5 to 1.5
- relax_rate: float32 [192, 1024], P('slab'), may hold values from 0.6 to 1.8
- perturbation: int32 [4, 192, 1024], P('ens', 'slab'), may hold values from -3 to 3
Outputs:
- lifted: float32 [4, 9, 192, 1024], P('ens', None, 'slab')
- projected: float32 [192, 1024], P('slab')
The draws below stay inside these ranges and needn't reach their ends.
All inputs are finite; a program needn't handle non-finite values.
Results may differ from the reference program's by a relative error of at most 0.0002.
Values sent between devices are 32-bit elements; how exact they have to be, the bound alone decides.
A program may use at most 64 MiB of HBM per device.

```python
import jax
import jax.numpy as jnp
from jax import lax

NC = 1024
MICRO_SPELLS = 3
STEPS = 8
MEMBERS = 4
NR = 192


def draw_density0(key, part):
    row_index = jnp.arange(NR, dtype=jnp.float32)
    row_ramp = 1.0 + 2.0 * row_index / max(NR - 1, 1)
    roughness = jax.random.truncated_normal(key, -4.0, 4.0, (NR, NC), jnp.float32)
    return 1.0 + 0.03 * row_ramp[:, None] * roughness


def set_ends(result, own_key, smallest, top_value):
    spot = [jax.random.randint(jax.random.fold_in(own_key, axis), (), 0, length) for axis, length in enumerate(result.shape)]
    longest = result.shape.index(max(result.shape))
    neighbour = spot[:longest] + [(spot[longest] + 1) % result.shape[longest]] + spot[longest + 1:]
    return result.at[tuple(spot)].set(smallest).at[tuple(neighbour)].set(top_value)


def levels(own_key, shape, shards, smallest, top_value):
    factor_of = 1.0
    for axis_at, shards_of in shards:
        steps = jax.random.uniform(jax.random.fold_in(jax.random.fold_in(own_key, 6), axis_at), (shards_of,), jnp.float32, smallest / len(shards), top_value / len(shards))
        factor_of = factor_of * jnp.repeat(jnp.exp(steps), shape[axis_at] // shards_of).reshape((-1,) + (1,) * (len(shape) - 1 - axis_at))
    return factor_of


def setup_inputs(seed: int = 0) -> dict:
    key_of = jax.random.split(jax.random.key(seed), 4)
    density0 = draw_density0(jax.random.fold_in(key_of[3], 71), 0)
    relax_rate = jnp.clip(0.6 + 1.1999999 * jax.random.uniform(key_of[1], (NR, NC), jnp.float32) ** levels(key_of[1], (NR, NC), ((0, 8),), -0.2, 0.2), 0.6, 1.8)
    perturbation = set_ends(jax.random.randint(key_of[2], (MEMBERS, NR, NC), -3, 4), jax.random.fold_in(key_of[2], 1), -3, 3).astype(jnp.int32)
    return {"density0": density0, "relax_rate": relax_rate, "perturbation": perturbation}


vertical_lattice_offsets = (0, 0, 1, 0, -1, 1, 1, -1, -1)
col_moves = (0, 1, 0, -1, 0, 1, -1, -1, 1)
lattice_weights = (4.0 / 9.0, 1.0 / 9.0, 1.0 / 9.0, 1.0 / 9.0, 1.0 / 9.0, 1.0 / 36.0, 1.0 / 36.0, 1.0 / 36.0, 1.0 / 36.0)
shift_amp = 0.08
step_cap = 0.25

def collide(distrib, relax_rate):
    density = distrib[..., 0, :, :]
    for direction in range(1, 9):
        density = density + distrib[..., direction, :, :]
    mom_row = distrib[..., 2, :, :] + distrib[..., 5, :, :] + distrib[..., 6, :, :] - (distrib[..., 4, :, :] + distrib[..., 7, :, :] + distrib[..., 8, :, :])
    mom_col = distrib[..., 1, :, :] + distrib[..., 5, :, :] + distrib[..., 8, :, :] - (distrib[..., 3, :, :] + distrib[..., 6, :, :] + distrib[..., 7, :, :])
    vel_row = mom_row / density
    vel_col = mom_col / density
    speed_sq = vel_row * vel_row + vel_col * vel_col
    relaxed = []
    for direction in range(9):
        along = vertical_lattice_offsets[direction] * vel_row + col_moves[direction] * vel_col
        equilib = lattice_weights[direction] * density * (1.0 + 3.0 * along + 4.5 * along * along - 1.5 * speed_sq)
        current = distrib[..., direction, :, :]
        relaxed.append(current - relax_rate * (current - equilib))
    return jnp.stack(relaxed, axis=-3)

def stream_full(relaxed):
    moved = [jnp.roll(relaxed[..., direction, :, :], (vertical_lattice_offsets[direction], col_moves[direction]), axis=(-2, -1)) for direction in range(9)]
    return jnp.stack(moved, axis=-3)

def reference(density0, relax_rate, perturbation):
    starts = density0[None] + shift_amp * perturbation.astype(jnp.float32)

    def advance_replica(start):
        distrib = jnp.stack([weight * start for weight in lattice_weights], axis=0)
        samples = []
        for spell_ordinal in range(MICRO_SPELLS):
            for step_index in range(STEPS):
                distrib = stream_full(collide(distrib, relax_rate))
            samples.append(lax.optimization_barrier(jnp.sum(distrib, axis=0)))
        return (distrib, jnp.stack(samples))
    finals, samples = lax.map(advance_replica, starts)
    totals = lax.optimization_barrier(jnp.sum(samples, axis=0))
    ensemble_mean = totals / MEMBERS
    first = ensemble_mean[0]
    middle = ensemble_mean[1]
    last = ensemble_mean[2]
    change = last - first
    fitted_slope = (first + middle + last) / 3.0 + 0.5 * change
    mean_square = jnp.sum(change * change) / (NR * NC)
    projected = fitted_slope + step_cap * change / jnp.sqrt(mean_square + 1e-06)
    lifted = finals * (projected[None] / samples[:, 2])[:, None]
    return (lifted, projected)
```

```python
import functools

import jax
import jax.numpy as jnp
from jax import lax
from jax.experimental import pallas as pl
from jax.experimental.pallas import tpu as pltpu
from jax.sharding import PartitionSpec as P

MICRO_SPELLS = 3
STEPS = 8
TOTAL = MICRO_SPELLS * STEPS
LANES = 128
CHUNK = 4

row_moves = (0, 0, 1, 0, -1, 1, 1, -1, -1)
col_moves = (0, 1, 0, -1, 0, 1, -1, -1, 1)
lattice_weights = (4.0 / 9.0,) + (1.0 / 9.0,) * 4 + (1.0 / 36.0,) * 4
shift_amp = 0.08
step_cap = 0.25
MESH = pl.DeviceIdType.MESH


def roll_columns(x, move):
    if move == 0:
        return x
    subs = x.shape[1]
    lane = lax.broadcasted_iota(jnp.int32, x.shape, 2)
    if move == 1:
        within = pltpu.roll(x, 1, 2)
        across = pltpu.roll(within, 1, 1)
        return jnp.where(lane == 0, across, within)
    within = pltpu.roll(x, LANES - 1, 2)
    across = pltpu.roll(within, subs - 1, 1)
    return jnp.where(lane == LANES - 1, across, within)


def collide(f, relax):
    s13, d13 = f[1] + f[3], f[1] - f[3]
    s24, d24 = f[2] + f[4], f[2] - f[4]
    s57, d57 = f[5] + f[7], f[5] - f[7]
    s68, d68 = f[6] + f[8], f[6] - f[8]
    density = (f[0] + (s13 + s24)) + (s57 + s68)
    mom_row = d24 + (d57 + d68)
    mom_col = d13 + (d57 - d68)
    inverse = 1.0 / density
    vel_row = mom_row * inverse
    vel_col = mom_col * inverse
    keep = 1.0 - relax
    third = relax * (1.0 / 3.0)
    third_row = third * mom_row
    third_col = third * mom_col
    half_rr = third_row * vel_row * 1.5
    half_cc = third_col * vel_col * 1.5
    quarter_rc = third_row * vel_col * 0.75
    squares = half_rr + half_cc
    base = (relax * density) * (1.0 / 9.0) - squares * (1.0 / 3.0)
    even_col = base + half_cc
    even_row = base + half_rr
    corner = 0.25 * (base + squares)
    even_57 = corner + quarter_rc
    even_68 = corner - quarter_rc
    odd_57 = 0.25 * (third_row + third_col)
    odd_68 = 0.25 * (third_row - third_col)
    k = [keep * value for value in f]
    return (
        k[0] + 4.0 * base,
        k[1] + (even_col + third_col),
        k[2] + (even_row + third_row),
        k[3] + (even_col - third_col),
        k[4] + (even_row - third_row),
        k[5] + (even_57 + odd_57),
        k[6] + (even_68 + odd_68),
        k[7] + (even_57 - odd_57),
        k[8] + (even_68 - odd_68),
    )


def kernel(
    ens,
    slabs,
    density_hbm,
    relax_hbm,
    pert_hbm,
    finals,
    last_rho,
    change_out,
    fitted_out,
    gain_out,
    density_in,
    relax_in,
    pert_in,
    start,
    relax,
    buf,
    gathered,
    squares,
    load_sem,
    halo_send,
    halo_recv,
    ens_send,
    ens_recv,
    sq_send,
    sq_recv,
):
    height, width = density_in.shape
    subs = width // LANES
    rows = height + 2 * TOTAL
    me_e = lax.axis_index("ens")
    me_s = lax.axis_index("slab")

    barrier = pltpu.get_barrier_semaphore()
    for k in range(1, ens):
        pl.semaphore_signal(
            barrier, inc=1, device_id={"ens": lax.rem(me_e + k, ens)}, device_id_type=MESH
        )
    for k in range(1, slabs):
        pl.semaphore_signal(
            barrier, inc=1, device_id={"slab": lax.rem(me_s + k, slabs)}, device_id_type=MESH
        )

    loads = [
        pltpu.make_async_copy(relax_hbm, relax_in, load_sem.at[0]),
        pltpu.make_async_copy(density_hbm, density_in, load_sem.at[1]),
        pltpu.make_async_copy(pert_hbm.at[0], pert_in, load_sem.at[2]),
    ]
    for load in loads:
        load.start()
    own = pl.ds(TOTAL, height)
    loads[0].wait()
    for s in range(subs):
        relax[own, s, :] = relax_in[:, s * LANES : (s + 1) * LANES]
    loads[1].wait()
    loads[2].wait()
    for s in range(subs):
        cols = slice(s * LANES, (s + 1) * LANES)
        start[own, s, :] = density_in[:, cols] + shift_amp * pert_in[:, cols].astype(jnp.float32)

    pl.semaphore_wait(barrier, ens + slabs - 2)
    right = lax.rem(me_s + 1, slabs)
    left = lax.rem(me_s + slabs - 1, slabs)
    halos = []
    for n, field in enumerate((relax, start)):
        for side, (target, source, dest) in enumerate(
            ((right, height, 0), (left, TOTAL, TOTAL + height))
        ):
            halos.append(
                pltpu.make_async_remote_copy(
                    src_ref=field.at[pl.ds(source, TOTAL)],
                    dst_ref=field.at[pl.ds(dest, TOTAL)],
                    send_sem=halo_send.at[n, side],
                    recv_sem=halo_recv.at[n, side],
                    device_id={"slab": target},
                    device_id_type=MESH,
                )
            )
    for copy in halos:
        copy.start()

    def first_rows(low, high):
        def body(c, carry):
            at = pl.ds(low + c * CHUNK, CHUNK)
            fresh = start[at]
            out = collide([weight * fresh for weight in lattice_weights], relax[at])
            for i in range(9):
                buf[1, i, at] = roll_columns(out[i], col_moves[i])
            return carry

        lax.fori_loop(0, (high - low) // CHUNK, body, 0)

    def step(k, carry):
        source, dest = lax.rem(k + 1, 2), lax.rem(k, 2)

        def body(c, inner):
            at = k - 1 + c * CHUNK
            f = [buf[source, i, pl.ds(at - row_moves[i], CHUNK)] for i in range(9)]
            out = collide(f, relax[pl.ds(at, CHUNK)])
            for i in range(9):
                buf[dest, i, pl.ds(at, CHUNK)] = roll_columns(out[i], col_moves[i])
            return inner

        lax.fori_loop(0, (rows - 2 * k + 2 + CHUNK - 1) // CHUNK, body, 0)
        return carry

    def spell_density(spell, parity):
        def body(c, inner):
            at = TOTAL + c * CHUNK
            total = buf[parity, 0, pl.ds(at, CHUNK)]
            for i in range(1, 9):
                total = total + buf[parity, i, pl.ds(at - row_moves[i], CHUNK)]
            gathered[spell, me_e, pl.ds(c * CHUNK, CHUNK)] = total
            return inner

        lax.fori_loop(0, height // CHUNK, body, 0)
        copies = []
        for k in range(1, ens):
            copies.append(
                pltpu.make_async_remote_copy(
                    src_ref=gathered.at[spell, me_e],
                    dst_ref=gathered.at[spell, me_e],
                    send_sem=ens_send.at[spell, k - 1],
                    recv_sem=ens_recv.at[spell, k - 1],
                    device_id={"ens": lax.rem(me_e + k, ens)},
                    device_id_type=MESH,
                )
            )
        for copy in copies:
            copy.start()
        return copies

    first_rows(TOTAL, TOTAL + height)
    for copy in halos:
        copy.wait_recv()
    first_rows(0, TOTAL)
    first_rows(TOTAL + height, rows)

    sent = []
    for spell in range(MICRO_SPELLS):
        lax.fori_loop(max(2, spell * STEPS + 1), (spell + 1) * STEPS + 1, step, 0)
        sent.append(spell_density(spell, ((spell + 1) * STEPS) % 2))

    parity = TOTAL % 2
    for s in range(subs):
        cols = slice(s * LANES, (s + 1) * LANES)
        for i in range(9):
            finals[i, :, cols] = buf[parity, i, pl.ds(TOTAL - row_moves[i], height), s, :]
        last_rho[:, cols] = gathered[MICRO_SPELLS - 1, me_e, :, s, :]

    for copies in sent:
        for copy in copies:
            copy.wait_recv()

    def mean(spell, at):
        total = gathered[spell, 0, at]
        for member in range(1, ens):
            total = total + gathered[spell, member, at]
        return total * (1.0 / ens)

    def fit(c, acc):
        at = pl.ds(c * CHUNK, CHUNK)
        first, middle, last = (mean(spell, at) for spell in range(MICRO_SPELLS))
        change = last - first
        start[at] = change
        relax[at] = (first + middle + last) * (1.0 / 3.0) + 0.5 * change
        return acc + jnp.sum(change * change, axis=0)

    acc = lax.fori_loop(0, height // CHUNK, fit, jnp.zeros((subs, LANES), jnp.float32))
    squares[me_s] = acc
    copies = []
    for k in range(1, slabs):
        copies.append(
            pltpu.make_async_remote_copy(
                src_ref=squares.at[me_s],
                dst_ref=squares.at[me_s],
                send_sem=sq_send.at[k - 1],
                recv_sem=sq_recv.at[k - 1],
                device_id={"slab": lax.rem(me_s + k, slabs)},
                device_id_type=MESH,
            )
        )
    for copy in copies:
        copy.start()
    for s in range(subs):
        cols = slice(s * LANES, (s + 1) * LANES)
        change_out[:, cols] = start[pl.ds(0, height), s, :]
        fitted_out[:, cols] = relax[pl.ds(0, height), s, :]
    for copy in copies:
        copy.wait_recv()
    total = jnp.sum(jnp.sum(squares[...], axis=0), axis=(0, 1), keepdims=True)
    mean_square = total * (1.0 / (height * width * slabs))
    gain = step_cap / jnp.sqrt(mean_square + 1e-06)
    gain_out[...] = jnp.broadcast_to(gain, gain_out.shape)

    for group in [halos, copies] + sent:
        for copy in group:
            copy.wait_send()


def on_device(density0, relax_rate, perturbation):
    height, width = density0.shape
    ens, slabs = lax.axis_size("ens"), lax.axis_size("slab")
    assert perturbation.shape[0] == 1 and height >= TOTAL and width % LANES == 0
    assert height % CHUNK == 0 and TOTAL % CHUNK == 0
    subs = width // LANES
    rows = height + 2 * TOTAL + CHUNK
    f32 = jnp.float32
    field = jax.ShapeDtypeStruct((height, width), f32)
    vmem = pl.BlockSpec(memory_space=pltpu.VMEM)
    dma = pltpu.SemaphoreType.DMA
    finals, last_rho, change, fitted, gain = pl.pallas_call(
        functools.partial(kernel, ens, slabs),
        out_shape=(
            jax.ShapeDtypeStruct((9, height, width), f32),
            field,
            field,
            field,
            jax.ShapeDtypeStruct((8, LANES), f32),
        ),
        in_specs=[pl.BlockSpec(memory_space=pl.ANY)] * 3,
        out_specs=[vmem] * 5,
        scratch_shapes=[
            pltpu.VMEM((height, width), f32),
            pltpu.VMEM((height, width), f32),
            pltpu.VMEM((height, width), jnp.int32),
            pltpu.VMEM((rows, subs, LANES), f32),
            pltpu.VMEM((rows, subs, LANES), f32),
            pltpu.VMEM((2, 9, rows, subs, LANES), f32),
            pltpu.VMEM((MICRO_SPELLS, ens, height, subs, LANES), f32),
            pltpu.VMEM((slabs, subs, LANES), f32),
            dma((3,)),
            dma((2, 2)),
            dma((2, 2)),
            dma((MICRO_SPELLS, ens - 1)),
            dma((MICRO_SPELLS, ens - 1)),
            dma((slabs - 1,)),
            dma((slabs - 1,)),
        ],
        compiler_params=pltpu.CompilerParams(collective_id=0, has_side_effects=True),
    )(density0, relax_rate, perturbation)
    projected = fitted + gain[0, 0] * change
    lifted = finals * (projected / last_rho)[None]
    return (lifted[None], projected)


def solution(mesh):
    in_specs = (P("slab", None), P("slab", None), P("ens", "slab", None))
    out_specs = (P("ens", None, "slab", None), P("slab", None))
    return jax.shard_map(
        on_device, mesh=mesh, in_specs=in_specs, out_specs=out_specs, check_vma=False
    )
```

```python
import functools

import jax
import jax.numpy as jnp
from jax import lax
from jax.experimental import pallas as pl
from jax.experimental.pallas import tpu as pltpu
from jax.sharding import PartitionSpec as P

MICRO_SPELLS = 3
STEPS = 8
TOTAL = MICRO_SPELLS * STEPS
LANES = 128
CHUNK = 4
BIG = 12
FIRST = 12
FRONT = 8

row_moves = (0, 0, 1, 0, -1, 1, 1, -1, -1)
col_moves = (0, 1, 0, -1, 0, 1, -1, -1, 1)
lattice_weights = (4.0 / 9.0,) + (1.0 / 9.0,) * 4 + (1.0 / 36.0,) * 4
shift_amp = 0.08
step_cap = 0.25
MESH = pl.DeviceIdType.MESH


def roll_columns(x, move):
    if move == 0:
        return x
    subs = x.shape[1]
    lane = lax.broadcasted_iota(jnp.int32, x.shape, 2)
    if move == 1:
        within = pltpu.roll(x, 1, 2)
        across = pltpu.roll(within, 1, 1)
        return jnp.where(lane == 0, across, within)
    within = pltpu.roll(x, LANES - 1, 2)
    across = pltpu.roll(within, subs - 1, 1)
    return jnp.where(lane == LANES - 1, across, within)


def collide(f, keep, third, ninth):
    s13, d13 = f[1] + f[3], f[1] - f[3]
    s24, d24 = f[2] + f[4], f[2] - f[4]
    s57, d57 = f[5] + f[7], f[5] - f[7]
    s68, d68 = f[6] + f[8], f[6] - f[8]
    density = (f[0] + (s13 + s24)) + (s57 + s68)
    mom_row = d24 + (d57 + d68)
    mom_col = d13 + (d57 - d68)
    inverse = 1.5 / density
    vel_row = mom_row * inverse
    vel_col = mom_col * inverse
    third_row = third * mom_row
    third_col = third * mom_col
    half_rr = third_row * vel_row
    half_cc = third_col * vel_col
    quarter_rc = (third_row * vel_col) * 0.5
    squares = half_rr + half_cc
    base = ninth * density - squares * (1.0 / 3.0)
    even_col = base + half_cc
    even_row = base + half_rr
    corner = 0.25 * (base + squares)
    even_57 = corner + quarter_rc
    even_68 = corner - quarter_rc
    odd_57 = 0.25 * (third_row + third_col)
    odd_68 = 0.25 * (third_row - third_col)
    k = [keep * value for value in f]
    return (
        k[0] + 4.0 * base,
        k[1] + (even_col + third_col),
        k[2] + (even_row + third_row),
        k[3] + (even_col - third_col),
        k[4] + (even_row - third_row),
        k[5] + (even_57 + odd_57),
        k[6] + (even_68 + odd_68),
        k[7] + (even_57 - odd_57),
        k[8] + (even_68 - odd_68),
    )


def kernel(
    ens,
    slabs,
    density_in,
    relax_in,
    pert_in,
    finals,
    scale_out,
    projected_out,
    start,
    relax,
    coef,
    buf,
    gathered,
    squares,
    halo_send,
    halo_recv,
    ens_send,
    ens_recv,
    sq_send,
    sq_recv,
):
    height, width = density_in.shape
    subs = width // LANES
    rows = height + 2 * TOTAL
    me_e = lax.axis_index("ens")
    me_s = lax.axis_index("slab")

    barrier = pltpu.get_barrier_semaphore()
    for k in range(1, ens):
        pl.semaphore_signal(
            barrier, inc=1, device_id={"ens": lax.rem(me_e + k, ens)}, device_id_type=MESH
        )
    for k in range(1, slabs):
        pl.semaphore_signal(
            barrier, inc=1, device_id={"slab": lax.rem(me_s + k, slabs)}, device_id_type=MESH
        )

    own = pl.ds(TOTAL, height)
    for s in range(subs):
        relax[own, s, :] = relax_in[:, s * LANES : (s + 1) * LANES]
    for s in range(subs):
        cols = slice(s * LANES, (s + 1) * LANES)
        start[own, s, :] = density_in[:, cols] + shift_amp * pert_in[0, :, cols].astype(jnp.float32)

    def first_rows(low, high):
        def body(c, carry):
            at = pl.ds(low + c * FIRST, FIRST)
            fresh = start[at]
            rate = relax[at]
            rates = (1.0 - rate, rate * (1.0 / 3.0), rate * (1.0 / 9.0))
            for n in range(3):
                coef[n, at] = rates[n]
            out = collide([weight * fresh for weight in lattice_weights], *rates)
            for i in range(9):
                buf[1, i, pl.ds(FRONT + low + c * FIRST, FIRST)] = roll_columns(out[i], col_moves[i])
            return carry

        lax.fori_loop(0, (high - low) // FIRST, body, 0)

    first_rows(TOTAL, TOTAL + height)
    pl.semaphore_wait(barrier, ens + slabs - 2)
    right = lax.rem(me_s + 1, slabs)
    left = lax.rem(me_s + slabs - 1, slabs)
    halos = []
    for n, field in enumerate((relax, start)):
        for side, (target, source, dest) in enumerate(
            ((right, height, 0), (left, TOTAL, TOTAL + height))
        ):
            halos.append(
                pltpu.make_async_remote_copy(
                    src_ref=field.at[pl.ds(source, TOTAL)],
                    dst_ref=field.at[pl.ds(dest, TOTAL)],
                    send_sem=halo_send.at[n, side],
                    recv_sem=halo_recv.at[n, side],
                    device_id={"slab": target},
                    device_id_type=MESH,
                )
            )
    for copy in halos:
        copy.start()

    def step(k, carry):
        source, dest = lax.rem(k + 1, 2), lax.rem(k, 2)

        def sweep(low, chunks, size):
            def body(c, inner):
                at = FRONT + low + c * size
                f = [buf[source, i, pl.ds(at - row_moves[i], size)] for i in range(9)]
                out = collide(f, *(coef[n, pl.ds(at - FRONT, size)] for n in range(3)))
                for i in range(9):
                    buf[dest, i, pl.ds(at, size)] = roll_columns(out[i], col_moves[i])
                return inner

            lax.fori_loop(0, chunks, body, 0)

        count = rows - 2 * k + 2
        whole = (count + CHUNK // 2) // BIG
        sweep(k - 1, whole, BIG)
        rest = jnp.maximum(count - whole * BIG, 0)
        sweep(k - 1 + whole * BIG, (rest + CHUNK - 1) // CHUNK, CHUNK)
        return carry

    def spell_density(spell, parity):
        def body(c, inner):
            at = FRONT + TOTAL + c * CHUNK
            total = buf[parity, 0, pl.ds(at, CHUNK)]
            for i in range(1, 9):
                total = total + buf[parity, i, pl.ds(at - row_moves[i], CHUNK)]
            gathered[spell, me_e, pl.ds(c * CHUNK, CHUNK)] = total
            return inner

        lax.fori_loop(0, height // CHUNK, body, 0)
        copies = []
        for k in range(1, ens):
            copies.append(
                pltpu.make_async_remote_copy(
                    src_ref=gathered.at[spell, me_e],
                    dst_ref=gathered.at[spell, me_e],
                    send_sem=ens_send.at[spell, k - 1],
                    recv_sem=ens_recv.at[spell, k - 1],
                    device_id={"ens": lax.rem(me_e + k, ens)},
                    device_id_type=MESH,
                )
            )
        for copy in copies:
            copy.start()
        return copies

    for copy in halos:
        copy.wait_recv()
    first_rows(0, TOTAL)
    first_rows(TOTAL + height, rows)

    sent = []
    for spell in range(MICRO_SPELLS):
        lax.fori_loop(max(2, spell * STEPS + 1), (spell + 1) * STEPS + 1, step, 0)
        sent.append(spell_density(spell, ((spell + 1) * STEPS) % 2))

    parity = TOTAL % 2
    for s in range(subs):
        cols = slice(s * LANES, (s + 1) * LANES)
        for i in range(9):
            finals[i, :, cols] = buf[parity, i, pl.ds(FRONT + TOTAL - row_moves[i], height), s, :]

    for copies in sent:
        for copy in copies:
            copy.wait_recv()

    def mean(spell, at):
        total = gathered[spell, 0, at]
        for member in range(1, ens):
            total = total + gathered[spell, member, at]
        return total * (1.0 / ens)

    def fit(c, acc):
        at = pl.ds(c * CHUNK, CHUNK)
        first, middle, last = (mean(spell, at) for spell in range(MICRO_SPELLS))
        change = last - first
        start[at] = change
        relax[at] = (first + middle + last) * (1.0 / 3.0) + 0.5 * change
        return acc + jnp.sum(change * change, axis=0)

    acc = lax.fori_loop(0, height // CHUNK, fit, jnp.zeros((subs, LANES), jnp.float32))
    squares[me_s] = acc
    copies = []
    for k in range(1, slabs):
        copies.append(
            pltpu.make_async_remote_copy(
                src_ref=squares.at[me_s],
                dst_ref=squares.at[me_s],
                send_sem=sq_send.at[k - 1],
                recv_sem=sq_recv.at[k - 1],
                device_id={"slab": lax.rem(me_s + k, slabs)},
                device_id_type=MESH,
            )
        )
    for copy in copies:
        copy.start()
    for copy in copies:
        copy.wait_recv()
    total = jnp.sum(jnp.sum(squares[...], axis=0), axis=(0, 1), keepdims=True)
    mean_square = total * (1.0 / (height * width * slabs))
    gain = (step_cap / jnp.sqrt(mean_square + 1e-06))[None]
    field = pl.ds(0, height)
    projected = relax[field] + gain * start[field]
    start[field] = projected
    relax[field] = projected / gathered[MICRO_SPELLS - 1, me_e]
    for s in range(subs):
        cols = slice(s * LANES, (s + 1) * LANES)
        projected_out[:, cols] = start[field, s, :]
        scale_out[:, cols] = relax[field, s, :]

    for group in [halos, copies] + sent:
        for copy in group:
            copy.wait_send()


def on_device(density0, relax_rate, perturbation):
    height, width = density0.shape
    ens, slabs = lax.axis_size("ens"), lax.axis_size("slab")
    assert perturbation.shape[0] == 1 and height >= TOTAL and width % LANES == 0
    assert height % CHUNK == 0 and CHUNK <= FRONT
    assert height % FIRST == 0 and TOTAL % FIRST == 0
    subs = width // LANES
    rows = height + 2 * TOTAL + max(CHUNK, FIRST)
    f32 = jnp.float32
    field = jax.ShapeDtypeStruct((height, width), f32)
    vmem = pl.BlockSpec(memory_space=pltpu.VMEM)
    dma = pltpu.SemaphoreType.DMA
    finals, scale, projected = pl.pallas_call(
        functools.partial(kernel, ens, slabs),
        out_shape=(
            jax.ShapeDtypeStruct((9, height, width), f32),
            field,
            field,
        ),
        in_specs=[vmem] * 3,
        out_specs=[vmem] * 3,
        scratch_shapes=[
            pltpu.VMEM((rows, subs, LANES), f32),
            pltpu.VMEM((rows, subs, LANES), f32),
            pltpu.VMEM((3, rows, subs, LANES), f32),
            pltpu.VMEM((2, 9, rows + FRONT, subs, LANES), f32),
            pltpu.VMEM((MICRO_SPELLS, ens, height, subs, LANES), f32),
            pltpu.VMEM((slabs, subs, LANES), f32),
            dma((2, 2)),
            dma((2, 2)),
            dma((MICRO_SPELLS, ens - 1)),
            dma((MICRO_SPELLS, ens - 1)),
            dma((slabs - 1,)),
            dma((slabs - 1,)),
        ],
        compiler_params=pltpu.CompilerParams(
            collective_id=0, has_side_effects=True, vmem_limit_bytes=24 << 20
        ),
    )(density0, relax_rate, perturbation)
    lifted = finals * scale[None]
    return (lifted[None], projected)


def solution(mesh):
    in_specs = (P("slab", None), P("slab", None), P("ens", "slab", None))
    out_specs = (P("ens", None, "slab", None), P("slab", None))
    return jax.shard_map(
        on_device, mesh=mesh, in_specs=in_specs, out_specs=out_specs, check_vma=False
    )
```
